32 devices in a mesh: dp: 8 (over z, x), tensor: 4 (over y, core).
Axes of the slice: x: 2, y: 2, z: 4, core: 2. Of those that a mesh axis runs over, the one named last changes fastest.
Arguments:
- residual: bfloat16 [2, 512, 5120], P(None, 'dp'), may hold values from -6 to 6
- context: bfloat16 [2, 512, 1536], P(None, 'dp', 'tensor'), may hold values from -6 to 6
- w_out: bfloat16 [1536, 5120], P('tensor'), may hold values from -0.15625 to 0.15625
- gain: float32 [5120], replicated, may hold values from 0.1 to 1.9
- cotangent: bfloat16 [2, 512, 5120], P(None, 'dp'), may hold values from -6 to 6
- slot_rows: int32 [4, 32], P('tensor'), may hold values from 0 to 383, as said below
Outputs:
- grad_slots: float32 [4, 5120, 32], P('tensor', 'dp')
- ctx_grad: bfloat16 [2, 512, 1536], P(None, 'dp', 'tensor')
- resid_grad: bfloat16 [2, 512, 5120], P(None, 'dp')
The draws below stay inside these ranges and needn't reach their ends.
Inputs may be any that keep to these rules, and one draw needn't show every extreme that they name: Each row of slot_rows holds 32 different numbers.
All inputs are finite; a program needn't handle non-finite values.
Results may differ from the reference program's by a relative error of at most 0.006.
Values may be sent and summed in bfloat16 or wider, within the bound.
A program may use at most 64 MiB of HBM per device.

```python
import jax
import jax.numpy as jnp
from jax import lax

DW = 5120
MICRO = 2
BUCKET = 32
HD_DEV = 384
HD = 1536
GROUPS = 4
REPLICAS = 8
TOKENS = 512


def draw_slot_rows(key, part):
    keys = jax.random.split(jax.random.fold_in(key, 7), GROUPS)
    rows = jax.vmap(lambda single: jax.random.permutation(single, HD_DEV))(keys)
    return rows[:, :BUCKET].astype(jnp.int32)


def raised(values, rng, source, target, shards_of, factor):
    owner, partner = [(jnp.arange(values.shape[position]) // (values.shape[position] // shards_of)).reshape([-1 if axis == position else 1 for axis in range(values.ndim)]) for position in (source, target)]
    chosen = jax.random.permutation(rng, shards_of)[partner]
    strong = (owner == chosen) | (owner == (partner + shards_of // 2) % shards_of)
    return jnp.where(strong, factor * values, values)


def block_levels(rng, dims, shards, least, high):
    level = 1.0
    for axis_at, shards_of in shards:
        steps = jax.random.uniform(jax.random.fold_in(jax.random.fold_in(rng, 6), axis_at), (shards_of,), jnp.float32, least / len(shards), high / len(shards))
        level = level * jnp.repeat(jnp.exp(steps), dims[axis_at] // shards_of).reshape((-1,) + (1,) * (len(dims) - 1 - axis_at))
    return level


def bell_draw(rng, shape, scale, reach, pieces=(), kind=jnp.bfloat16):
    drawn = scale * jax.random.normal(rng, shape, jnp.float32)
    if pieces:
        drawn = drawn * block_levels(rng, shape, pieces, -0.22, 0.18)
    return jnp.clip(drawn, -reach, reach).astype(kind)


def gaussian_with(key, shape, spread, limit, cuts, heavy, dtype=jnp.bfloat16):
    values = spread * jax.random.normal(key, shape, jnp.float32)
    if cuts:
        values = values * block_levels(key, shape, cuts, -0.22, 0.18)
    return jnp.clip(raised(values, jax.random.fold_in(key, 3), *heavy), -limit, limit).astype(dtype)


def setup_inputs(seed: int = 0) -> dict:
    key_of = jax.random.split(jax.random.key(seed), 7)
    return {
        "residual": bell_draw(key_of[0], (MICRO, TOKENS, DW), 1.0, 6.0, ((1, 8),)),
        "context": gaussian_with(key_of[1], (MICRO, TOKENS, HD), 1.0, 6.0, ((1, 8), (2, 4)), (1, 2, 8, 2.0)),
        "w_out": bell_draw(key_of[2], (HD, DW), HD ** -0.5, 0.15625, ((0, 4),)),
        "gain": jnp.clip(1.0 + 0.18 * jax.random.normal(key_of[3], (DW,), jnp.float32), 0.1, 1.9),
        "cotangent": bell_draw(key_of[4], (MICRO, TOKENS, DW), 1.0, 6.0, ((1, 8),)),
        "slot_rows": draw_slot_rows(jax.random.fold_in(key_of[6], 71), 0),
    }


def norm_backward(res_rows, summed, gain, cot_rows):
    hidden = res_rows.astype(jnp.float32) + summed
    center = hidden - lax.optimization_barrier(jnp.mean(hidden, axis=-1, keepdims=True))
    inverse = lax.rsqrt(lax.optimization_barrier(jnp.mean(center * center, axis=-1, keepdims=True)) + 1e-05)
    normed = center * inverse
    upstream = cot_rows.astype(jnp.float32) * gain
    result = inverse * (upstream - lax.optimization_barrier(jnp.mean(upstream, axis=-1, keepdims=True)) - normed * lax.optimization_barrier(jnp.mean(upstream * normed, axis=-1, keepdims=True)))
    return result.astype(jnp.bfloat16)

def reference(residual, context, w_out, gain, cotangent, slot_rows):
    groups = slot_rows.shape[0]
    width = w_out.shape[0] // groups
    gradient = jnp.zeros((w_out.shape[0], w_out.shape[1]), jnp.float32)
    resid_list = []
    ctx_list = []
    for micro_idx in range(residual.shape[0]):
        ctx_rows = context[micro_idx]
        summed = jnp.zeros(residual.shape[1:], jnp.float32)
        for group_idx in range(groups):
            first_row = group_idx * width
            partial_value = jnp.dot(ctx_rows[:, first_row:first_row + width], w_out[first_row:first_row + width], preferred_element_type=jnp.float32)
            summed = summed + lax.optimization_barrier(partial_value.astype(jnp.bfloat16)).astype(jnp.float32)
        grad_rows = norm_backward(residual[micro_idx], summed, gain, cotangent[micro_idx])
        resid_list.append(grad_rows)
        ctx_back = lax.dot_general(grad_rows, w_out, (((1,), (1,)), ((), ())), preferred_element_type=jnp.float32)
        ctx_list.append(ctx_back.astype(jnp.bfloat16))
        gradient = gradient + lax.dot_general(ctx_rows, grad_rows, (((0,), (0,)), ((), ())), preferred_element_type=jnp.float32)
    gradient = gradient / REPLICAS
    slots = jnp.take_along_axis(gradient.reshape(groups, width, -1), slot_rows[:, :, None], axis=1)
    return (jnp.transpose(slots, (0, 2, 1)), jnp.stack(ctx_list), jnp.stack(resid_list))
```

```python
import functools

import jax
import jax.numpy as jnp
from jax import lax
from jax.experimental import pallas as pl
from jax.experimental.pallas import tpu as pltpu
from jax.sharding import PartitionSpec as P

MESH = pl.DeviceIdType.MESH
ANY = pl.BlockSpec(memory_space=pl.ANY)
VMEM = pl.BlockSpec(memory_space=pltpu.VMEM)
F32 = jnp.float32
BF16 = jnp.bfloat16
LANES = 128
ROWS = 16


def pieces_of(width):
    for count in (4, 2):
        if width % (count * LANES) == 0:
            return count
    return 1


def norm_backward(hidden, cot_rows, gain):
    scale = 1.0 / hidden.shape[-1]
    center = hidden - jnp.sum(hidden, axis=-1, keepdims=True) * scale
    inverse = lax.rsqrt(jnp.sum(center * center, axis=-1, keepdims=True) * scale + 1e-05)
    upstream = cot_rows.astype(F32) * gain
    mean_up = jnp.sum(upstream, axis=-1, keepdims=True) * scale
    slope = jnp.sum(upstream * center, axis=-1, keepdims=True) * scale * inverse * inverse
    return (inverse * (upstream - mean_up - center * slope)).astype(BF16)


def kernel(reduce_dp, replicas, tensors, res_hbm, ctx_hbm, w_hbm, gain_hbm, cot_hbm, slot_ref,
           slots_out, ctx_out, resid_out,
           ctx, w, res, cot, gain, lhs, psend, precv, own, ysum, resid, gsend, grecv, gown,
           load_sem, w_sem, store_sem, p_send, p_recv, y_send, y_recv, r_send, r_recv, g_send, g_recv):
    rows, width = resid.shape
    half = rows // 2
    chips = tensors // 2
    dp = lax.axis_index("dp")
    tensor = lax.axis_index("tensor")
    chip, core = tensor // 2, tensor % 2
    mate = chip * 2 + (1 - core)
    mine = pl.multiple_of(core * half, half)
    theirs = pl.multiple_of((1 - core) * half, half)
    count = pieces_of(width)
    cols = width // count
    chunks = half // ROWS
    bucket = slot_ref.shape[1]

    load_ctx = pltpu.make_async_copy(ctx_hbm, ctx, load_sem.at[0])
    load_ctx.start()
    loads_w = []
    for j in range(count):
        span = pl.ds(j * cols, cols)
        copy = pltpu.make_async_copy(w_hbm.at[:, span], w.at[:, span], w_sem.at[j])
        copy.start()
        loads_w.append(copy)
    load_rest = [
        pltpu.make_async_copy(res_hbm.at[pl.ds(mine, half)], res, load_sem.at[1]),
        pltpu.make_async_copy(cot_hbm.at[pl.ds(mine, half)], cot, load_sem.at[2]),
        pltpu.make_async_copy(gain_hbm, gain, load_sem.at[3]),
    ]
    for copy in load_rest:
        copy.start()

    barrier = pltpu.get_barrier_semaphore()
    pl.semaphore_signal(barrier, inc=1, device_id={"dp": dp, "tensor": mate}, device_id_type=MESH)
    greeted = 1
    for i in range(1, chips):
        other = lax.rem(chip + i, chips) * 2 + core
        pl.semaphore_signal(barrier, inc=1, device_id={"dp": dp, "tensor": other}, device_id_type=MESH)
        greeted += 1
    if reduce_dp:
        for i in range(1, replicas):
            pl.semaphore_signal(barrier, inc=1, device_id={"dp": lax.rem(dp + i, replicas), "tensor": tensor},
                                device_id_type=MESH)
            greeted += 1

    load_ctx.wait()
    lhs[pl.ds(0, half)] = ctx[pl.ds(theirs, half)]
    lhs[pl.ds(half, half)] = ctx[pl.ds(mine, half)]

    def to_mate(j):
        span = pl.ds(j * cols, cols)
        return pltpu.make_async_remote_copy(
            src_ref=psend.at[:, span], dst_ref=precv.at[:, span], send_sem=p_send.at[j], recv_sem=p_recv.at[j],
            device_id={"dp": dp, "tensor": mate}, device_id_type=MESH)

    for j in range(count):
        span = pl.ds(j * cols, cols)
        loads_w[j].wait()
        product = jnp.dot(lhs[...], w[:, span], preferred_element_type=F32)
        psend[:, span] = product[:half].astype(BF16)
        own[:, span] = product[half:]
        if j == 0:
            pl.semaphore_wait(barrier, greeted)
        to_mate(j).start()

    def across(i, piece):
        other = lax.rem(chip + i, chips) * 2 + core
        if piece < count:
            block = ysum.at[chip, pl.ds(0, ROWS), pl.ds(piece * cols, cols)]
        else:
            block = ysum.at[chip, pl.ds((piece - count + 1) * ROWS, ROWS)]
        return pltpu.make_async_remote_copy(
            src_ref=block, dst_ref=block, send_sem=y_send.at[i - 1, piece], recv_sem=y_recv.at[i - 1, piece],
            device_id={"dp": dp, "tensor": other}, device_id_type=MESH)

    total = count + chunks - 1
    for j in range(count):
        span = pl.ds(j * cols, cols)
        to_mate(j).wait_recv()
        ysum[chip, :, span] = (own[:, span] + precv[:, span].astype(F32)).astype(BF16)
        for i in range(1, chips):
            across(i, j).start()
    for piece in range(count, total):
        for i in range(1, chips):
            across(i, piece).start()

    square = (bucket, bucket)
    diagonal = lax.broadcasted_iota(jnp.int32, square, 0) == lax.broadcasted_iota(jnp.int32, square, 1)
    order = jnp.sum(jnp.where(diagonal, slot_ref[...].astype(F32), 0.0), axis=1, keepdims=True)
    place = lax.broadcasted_iota(jnp.int32, (bucket, ctx.shape[1]), 1).astype(F32)
    chosen = jnp.where(place == order, 1.0, 0.0).astype(BF16)
    picked = lax.dot_general(chosen, ctx[...], (((1,), (1,)), ((), ())),
                             preferred_element_type=F32).astype(BF16)

    def share(r):
        span = pl.ds(mine + r * ROWS, ROWS)
        return pltpu.make_async_remote_copy(
            src_ref=resid.at[span], dst_ref=resid.at[span], send_sem=r_send.at[r], recv_sem=r_recv.at[r],
            device_id={"dp": dp, "tensor": mate}, device_id_type=MESH)

    for copy in load_rest:
        copy.wait()
    for r in range(chunks):
        for piece in (range(count) if r == 0 else (count + r - 1,)):
            for i in range(1, chips):
                across(i, piece).wait_recv()
        span = pl.ds(r * ROWS, ROWS)
        summed = ysum[0, span].astype(F32)
        for k in range(1, chips):
            summed = summed + ysum[k, span].astype(F32)
        hidden = res[span].astype(F32) + summed
        resid[pl.ds(pl.multiple_of(mine + r * ROWS, ROWS), ROWS)] = norm_backward(hidden, cot[span], gain[...])
        share(r).start()
    for r in range(chunks):
        share(r).wait_recv()
    store_resid = pltpu.make_async_copy(resid, resid_out, store_sem.at[0])
    store_resid.start()

    def to_peer(i):
        return pltpu.make_async_remote_copy(
            src_ref=gsend.at[i - 1], dst_ref=grecv.at[i - 1], send_sem=g_send.at[i - 1], recv_sem=g_recv.at[i - 1],
            device_id={"dp": lax.rem(dp + i, replicas), "tensor": tensor}, device_id_type=MESH)

    if reduce_dp:
        block = width // replicas
        for i in list(range(1, replicas)) + [0]:
            span = pl.ds(pl.multiple_of(lax.rem(dp + i, replicas) * block, block), block)
            gradient = jnp.dot(picked, resid[:, span], preferred_element_type=F32)
            if i == 0:
                gown[...] = gradient
            else:
                gsend[i - 1] = gradient.astype(BF16)
                to_peer(i).start()
    else:
        for j in range(count):
            span = pl.ds(j * cols, cols)
            slots_out[:, span] = jnp.dot(picked, resid[:, span], preferred_element_type=F32)

    back = None
    for j in range(count):
        span = pl.ds(j * cols, cols)
        term = lax.dot_general(resid[:, span], w[:, span], (((1,), (1,)), ((), ())), preferred_element_type=F32)
        back = term if back is None else back + term
    ctx_out[...] = back.astype(BF16)

    if reduce_dp:
        gradient = gown[...]
        for i in range(1, replicas):
            to_peer(i).wait_recv()
            gradient = gradient + grecv[i - 1].astype(F32)
        slots_out[...] = gradient * (1.0 / replicas)
    for j in range(count):
        to_mate(j).wait_send()
    for piece in range(total):
        for i in range(1, chips):
            across(i, piece).wait_send()
    for r in range(chunks):
        share(r).wait_send()
    if reduce_dp:
        for i in range(1, replicas):
            to_peer(i).wait_send()
    store_resid.wait()


def body(replicas, tensors, residual, context, w_out, gain, cotangent, slot_rows):
    micro, tokens, width = residual.shape
    depth = w_out.shape[0]
    bucket = slot_rows.shape[1]
    rows = micro * tokens
    half = rows // 2
    chips = tensors // 2
    count = pieces_of(width)
    pieces = count + half // ROWS - 1
    reduce_dp = width % (replicas * LANES) == 0
    block = width // replicas if reduce_dp else LANES
    peers = max(replicas - 1, 1) if reduce_dp else 1
    dma = pltpu.SemaphoreType.DMA
    slots, ctx_grad, resid = pl.pallas_call(
        functools.partial(kernel, reduce_dp, replicas, tensors),
        out_shape=(
            jax.ShapeDtypeStruct((bucket, block if reduce_dp else width), F32),
            jax.ShapeDtypeStruct((rows, depth), BF16),
            jax.ShapeDtypeStruct((rows, width), BF16),
        ),
        in_specs=[ANY] * 5 + [VMEM],
        out_specs=(VMEM, VMEM, ANY),
        scratch_shapes=[
            pltpu.VMEM((rows, depth), BF16),
            pltpu.VMEM((depth, width), BF16),
            pltpu.VMEM((half, width), BF16),
            pltpu.VMEM((half, width), BF16),
            pltpu.VMEM((1, width), F32),
            pltpu.VMEM((rows, depth), BF16),
            pltpu.VMEM((half, width), BF16),
            pltpu.VMEM((half, width), BF16),
            pltpu.VMEM((half, width), F32),
            pltpu.VMEM((chips, half, width), BF16),
            pltpu.VMEM((rows, width), BF16),
            pltpu.VMEM((peers, bucket, block), BF16),
            pltpu.VMEM((peers, bucket, block), BF16),
            pltpu.VMEM((bucket, block), F32),
            dma((4,)), dma((count,)), dma((1,)), dma((count,)), dma((count,)),
            dma((max(chips - 1, 1), pieces)), dma((max(chips - 1, 1), pieces)),
            dma((half // ROWS,)), dma((half // ROWS,)), dma((peers,)), dma((peers,)),
        ],
        compiler_params=pltpu.CompilerParams(
            collective_id=0, has_side_effects=True, vmem_limit_bytes=60 * 1024 * 1024),
    )(residual.reshape(rows, width), context.reshape(rows, depth), w_out, gain.reshape(1, width),
      cotangent.reshape(rows, width), slot_rows)
    if not reduce_dp:
        slots = lax.psum_scatter(slots, "dp", scatter_dimension=1, tiled=True) / replicas
    return (slots.T[None], ctx_grad.reshape(micro, tokens, depth), resid.reshape(micro, tokens, width))


def solution(mesh):
    in_specs = (
        P(None, "dp", None),
        P(None, "dp", "tensor"),
        P("tensor", None),
        P(),
        P(None, "dp", None),
        P("tensor", None),
    )
    out_specs = (P("tensor", "dp", None), P(None, "dp", "tensor"), P(None, "dp", None))
    step = functools.partial(body, mesh.shape["dp"], mesh.shape["tensor"])
    return jax.shard_map(step, mesh=mesh, in_specs=in_specs, out_specs=out_specs, check_vma=False)
```

```python
import functools

import jax
import jax.numpy as jnp
from jax import lax
from jax.experimental import pallas as pl
from jax.experimental.pallas import tpu as pltpu
from jax.sharding import PartitionSpec as P

MESH = pl.DeviceIdType.MESH
ANY = pl.BlockSpec(memory_space=pl.ANY)
VMEM = pl.BlockSpec(memory_space=pltpu.VMEM)
F32 = jnp.float32
BF16 = jnp.bfloat16
LANES = 128
ROWS = 16
VMEM_BYTES = 67043328


def pieces_of(width):
    for count in (4, 2):
        if width % (count * LANES) == 0:
            return count
    return 1


def norm_backward(hidden, cot_rows, gain):
    scale = 1.0 / hidden.shape[-1]
    center = hidden - jnp.sum(hidden, axis=-1, keepdims=True) * scale
    inverse = lax.rsqrt(jnp.sum(center * center, axis=-1, keepdims=True) * scale + 1e-05)
    upstream = cot_rows.astype(F32) * gain
    mean_up = jnp.sum(upstream, axis=-1, keepdims=True) * scale
    slope = jnp.sum(upstream * center, axis=-1, keepdims=True) * scale * inverse * inverse
    return (inverse * (upstream - mean_up - center * slope)).astype(BF16)


def kernel(reduce_dp, replicas, tensors, res_hbm, ctx_hbm, w_hbm, gain_hbm, cot_hbm, slot_ref,
           slots_out, ctx_out, resid,
           ctx, w, res, cot, gain, lhs, psend, precv, own, ysum, gsend, grecv, gown,
           load_sem, w_sem, p_send, p_recv, y_send, y_recv, r_send, r_recv, g_send, g_recv):
    rows, width = resid.shape
    half = rows // 2
    chips = tensors // 2
    dp = lax.axis_index("dp")
    tensor = lax.axis_index("tensor")
    chip, core = tensor // 2, tensor % 2
    mate = chip * 2 + (1 - core)
    mine = pl.multiple_of(core * half, half)
    theirs = pl.multiple_of((1 - core) * half, half)
    count = pieces_of(width)
    cols = width // count
    chunks = half // ROWS
    bucket = slot_ref.shape[1]

    load_ctx = pltpu.make_async_copy(ctx_hbm, ctx, load_sem.at[0])
    load_ctx.start()
    loads_w = []
    for j in range(count):
        span = pl.ds(j * cols, cols)
        copy = pltpu.make_async_copy(w_hbm.at[:, span], w.at[:, span], w_sem.at[j])
        copy.start()
        loads_w.append(copy)
    load_rest = [
        pltpu.make_async_copy(res_hbm.at[pl.ds(mine, half)], res, load_sem.at[1]),
        pltpu.make_async_copy(cot_hbm.at[pl.ds(mine, half)], cot, load_sem.at[2]),
        pltpu.make_async_copy(gain_hbm, gain, load_sem.at[3]),
    ]
    for copy in load_rest:
        copy.start()

    barrier = pltpu.get_barrier_semaphore()
    pl.semaphore_signal(barrier, inc=1, device_id={"dp": dp, "tensor": mate}, device_id_type=MESH)
    greeted = 1
    for i in range(1, chips):
        other = lax.rem(chip + i, chips) * 2 + core
        pl.semaphore_signal(barrier, inc=1, device_id={"dp": dp, "tensor": other}, device_id_type=MESH)
        greeted += 1
    if reduce_dp:
        for i in range(1, replicas):
            pl.semaphore_signal(barrier, inc=1, device_id={"dp": lax.rem(dp + i, replicas), "tensor": tensor},
                                device_id_type=MESH)
            greeted += 1

    load_ctx.wait()
    lhs[pl.ds(0, half)] = ctx[pl.ds(theirs, half)]
    lhs[pl.ds(half, half)] = ctx[pl.ds(mine, half)]

    def to_mate(j):
        span = pl.ds(j * cols, cols)
        return pltpu.make_async_remote_copy(
            src_ref=psend.at[:, span], dst_ref=precv.at[:, span], send_sem=p_send.at[j], recv_sem=p_recv.at[j],
            device_id={"dp": dp, "tensor": mate}, device_id_type=MESH)

    for j in range(count):
        span = pl.ds(j * cols, cols)
        loads_w[j].wait()
        product = jnp.dot(lhs[...], w[:, span], preferred_element_type=F32)
        psend[:, span] = product[:half].astype(BF16)
        own[:, span] = product[half:]
        if j == 0:
            pl.semaphore_wait(barrier, greeted)
        to_mate(j).start()

    def across(i, piece):
        other = lax.rem(chip + i, chips) * 2 + core
        if piece < count:
            block = ysum.at[chip, pl.ds(0, ROWS), pl.ds(piece * cols, cols)]
        else:
            block = ysum.at[chip, pl.ds((piece - count + 1) * ROWS, ROWS)]
        return pltpu.make_async_remote_copy(
            src_ref=block, dst_ref=block, send_sem=y_send.at[i - 1, piece], recv_sem=y_recv.at[i - 1, piece],
            device_id={"dp": dp, "tensor": other}, device_id_type=MESH)

    total = count + chunks - 1
    for j in range(count):
        span = pl.ds(j * cols, cols)
        to_mate(j).wait_recv()
        ysum[chip, :, span] = (own[:, span] + precv[:, span].astype(F32)).astype(BF16)
        for i in range(1, chips):
            across(i, j).start()
    for piece in range(count, total):
        for i in range(1, chips):
            across(i, piece).start()

    square = (bucket, bucket)
    diagonal = lax.broadcasted_iota(jnp.int32, square, 0) == lax.broadcasted_iota(jnp.int32, square, 1)
    order = jnp.sum(jnp.where(diagonal, slot_ref[...].astype(F32), 0.0), axis=1, keepdims=True)
    place = lax.broadcasted_iota(jnp.int32, (bucket, ctx.shape[1]), 1).astype(F32)
    chosen = jnp.where(place == order, 1.0, 0.0).astype(BF16)
    picked = lax.dot_general(chosen, ctx[...], (((1,), (1,)), ((), ())),
                             preferred_element_type=F32).astype(BF16)

    def share(r):
        span = pl.ds(mine + r * ROWS, ROWS)
        return pltpu.make_async_remote_copy(
            src_ref=resid.at[span], dst_ref=resid.at[span], send_sem=r_send.at[r], recv_sem=r_recv.at[r],
            device_id={"dp": dp, "tensor": mate}, device_id_type=MESH)

    for copy in load_rest:
        copy.wait()
    for r in range(chunks):
        for piece in (range(count) if r == 0 else (count + r - 1,)):
            for i in range(1, chips):
                across(i, piece).wait_recv()
        span = pl.ds(r * ROWS, ROWS)
        summed = ysum[0, span].astype(F32)
        for k in range(1, chips):
            summed = summed + ysum[k, span].astype(F32)
        hidden = res[span].astype(F32) + summed
        resid[pl.ds(pl.multiple_of(mine + r * ROWS, ROWS), ROWS)] = norm_backward(hidden, cot[span], gain[...])
        share(r).start()
    for r in range(chunks):
        share(r).wait_recv()

    def to_peer(i):
        return pltpu.make_async_remote_copy(
            src_ref=gsend.at[i - 1], dst_ref=grecv.at[i - 1], send_sem=g_send.at[i - 1], recv_sem=g_recv.at[i - 1],
            device_id={"dp": lax.rem(dp + i, replicas), "tensor": tensor}, device_id_type=MESH)

    if reduce_dp:
        block = width // replicas
        for i in list(range(1, replicas)) + [0]:
            span = pl.ds(pl.multiple_of(lax.rem(dp + i, replicas) * block, block), block)
            gradient = jnp.dot(picked, resid[:, span], preferred_element_type=F32)
            if i == 0:
                gown[...] = gradient
            else:
                gsend[i - 1] = gradient.astype(BF16)
                to_peer(i).start()
    else:
        for j in range(count):
            span = pl.ds(j * cols, cols)
            slots_out[:, span] = jnp.dot(picked, resid[:, span], preferred_element_type=F32)

    back = None
    for j in range(count):
        span = pl.ds(j * cols, cols)
        term = lax.dot_general(resid[:, span], w[:, span], (((1,), (1,)), ((), ())), preferred_element_type=F32)
        back = term if back is None else back + term
    ctx_out[...] = back.astype(BF16)

    if reduce_dp:
        gradient = gown[...]
        for i in range(1, replicas):
            to_peer(i).wait_recv()
            gradient = gradient + grecv[i - 1].astype(F32)
        slots_out[...] = gradient * (1.0 / replicas)
    for j in range(count):
        to_mate(j).wait_send()
    for piece in range(total):
        for i in range(1, chips):
            across(i, piece).wait_send()
    for r in range(chunks):
        share(r).wait_send()
    if reduce_dp:
        for i in range(1, replicas):
            to_peer(i).wait_send()


def store_kernel(count, *refs):
    copies = [pltpu.make_async_copy(refs[i], refs[count + i], refs[2 * count].at[i]) for i in range(count)]
    for copy in copies:
        copy.start()
    for copy in copies:
        copy.wait()


def store(*arrays):
    count = len(arrays)
    return pl.pallas_call(
        functools.partial(store_kernel, count),
        out_shape=tuple(jax.ShapeDtypeStruct(a.shape, a.dtype) for a in arrays),
        in_specs=[ANY] * count,
        out_specs=(ANY,) * count,
        scratch_shapes=[pltpu.SemaphoreType.DMA((count,))],
        compiler_params=pltpu.CompilerParams(vmem_limit_bytes=1024 * 1024),
    )(*arrays)


def body(replicas, tensors, residual, context, w_out, gain, cotangent, slot_rows):
    micro, tokens, width = residual.shape
    depth = w_out.shape[0]
    bucket = slot_rows.shape[1]
    rows = micro * tokens
    half = rows // 2
    chips = tensors // 2
    count = pieces_of(width)
    pieces = count + half // ROWS - 1
    reduce_dp = width % (replicas * LANES) == 0
    block = width // replicas if reduce_dp else LANES
    peers = max(replicas - 1, 1) if reduce_dp else 1
    dma = pltpu.SemaphoreType.DMA
    spare = 4 * bucket * (block if reduce_dp else width) + 2 * rows * (depth + width)
    slots, ctx_grad, resid = pl.pallas_call(
        functools.partial(kernel, reduce_dp, replicas, tensors),
        out_shape=(
            pltpu.VMEM((bucket, block if reduce_dp else width), F32),
            pltpu.VMEM((rows, depth), BF16),
            pltpu.VMEM((rows, width), BF16),
        ),
        in_specs=[ANY] * 5 + [VMEM],
        out_specs=(VMEM, VMEM, VMEM),
        scratch_shapes=[
            pltpu.VMEM((rows, depth), BF16),
            pltpu.VMEM((depth, width), BF16),
            pltpu.VMEM((half, width), BF16),
            pltpu.VMEM((half, width), BF16),
            pltpu.VMEM((1, width), F32),
            pltpu.VMEM((rows, depth), BF16),
            pltpu.VMEM((half, width), BF16),
            pltpu.VMEM((half, width), BF16),
            pltpu.VMEM((half, width), F32),
            pltpu.VMEM((chips, half, width), BF16),
            pltpu.VMEM((peers, bucket, block), BF16),
            pltpu.VMEM((peers, bucket, block), BF16),
            pltpu.VMEM((bucket, block), F32),
            dma((4,)), dma((count,)), dma((count,)), dma((count,)),
            dma((max(chips - 1, 1), pieces)), dma((max(chips - 1, 1), pieces)),
            dma((half // ROWS,)), dma((half // ROWS,)), dma((peers,)), dma((peers,)),
        ],
        compiler_params=pltpu.CompilerParams(
            collective_id=0, has_side_effects=True, vmem_limit_bytes=VMEM_BYTES - spare),
    )(residual.reshape(rows, width), context.reshape(rows, depth), w_out, gain.reshape(1, width),
      cotangent.reshape(rows, width), slot_rows)
    slots, ctx_grad, resid = store(slots, ctx_grad, resid)
    if not reduce_dp:
        slots = lax.psum_scatter(slots, "dp", scatter_dimension=1, tiled=True) / replicas
    return (slots.T[None], ctx_grad.reshape(micro, tokens, depth), resid.reshape(micro, tokens, width))


def solution(mesh):
    in_specs = (
        P(None, "dp", None),
        P(None, "dp", "tensor"),
        P("tensor", None),
        P(),
        P(None, "dp", None),
        P("tensor", None),
    )
    out_specs = (P("tensor", "dp", None), P(None, "dp", "tensor"), P(None, "dp", None))
    step = functools.partial(body, mesh.shape["dp"], mesh.shape["tensor"])
    return jax.shard_map(step, mesh=mesh, in_specs=in_specs, out_specs=out_specs, check_vma=False)
```

```python
import functools

import jax
import jax.numpy as jnp
from jax import lax
from jax.experimental import pallas as pl
from jax.experimental.pallas import tpu as pltpu
from jax.sharding import PartitionSpec as P

MESH = pl.DeviceIdType.MESH
ANY = pl.BlockSpec(memory_space=pl.ANY)
VMEM = pl.BlockSpec(memory_space=pltpu.VMEM)
F32 = jnp.float32
BF16 = jnp.bfloat16
LANES = 128
ROWS = 16
VMEM_BYTES = 67043328


def pieces_of(width):
    for count in (8, 4, 2):
        if width % (count * LANES) == 0:
            return count
    return 1


def norm_backward(hidden, cot_rows, gain):
    scale = 1.0 / hidden.shape[-1]
    center = hidden - jnp.sum(hidden, axis=-1, keepdims=True) * scale
    inverse = lax.rsqrt(jnp.sum(center * center, axis=-1, keepdims=True) * scale + 1e-05)
    upstream = cot_rows.astype(F32) * gain
    mean_up = jnp.sum(upstream, axis=-1, keepdims=True) * scale
    slope = jnp.sum(upstream * center, axis=-1, keepdims=True) * scale * inverse * inverse
    return (inverse * (upstream - mean_up - center * slope)).astype(BF16)


def kernel(reduce_dp, replicas, tensors, res_hbm, ctx_hbm, w_hbm, gain_hbm, cot_hbm, slot_ref,
           slots_out, ctx_out, resid,
           ctx, w, res, cot, gain, lhs, psend, precv, own, ysum, gsend, grecv, gown,
           load_sem, w_sem, p_send, p_recv, y_send, y_recv, r_send, r_recv, g_send, g_recv, ladder):
    rows, width = resid.shape
    half = rows // 2
    chips = tensors // 2
    dp = lax.axis_index("dp")
    tensor = lax.axis_index("tensor")
    chip, core = tensor // 2, tensor % 2
    mate = chip * 2 + (1 - core)
    mine = pl.multiple_of(core * half, half)
    theirs = pl.multiple_of((1 - core) * half, half)
    count = pieces_of(width)
    cols = width // count
    chunks = half // ROWS
    bucket = slot_ref.shape[1]

    load_ctx = pltpu.make_async_copy(ctx_hbm, ctx, load_sem.at[0])
    load_ctx.start()
    loads_w = []
    for j in range(count):
        span = pl.ds(j * cols, cols)
        copy = pltpu.make_async_copy(w_hbm.at[:, span], w.at[:, span], w_sem.at[j])
        copy.start()
        loads_w.append(copy)
    load_rest = [
        pltpu.make_async_copy(res_hbm.at[pl.ds(mine, half)], res, load_sem.at[1]),
        pltpu.make_async_copy(cot_hbm.at[pl.ds(mine, half)], cot, load_sem.at[2]),
        pltpu.make_async_copy(gain_hbm, gain, load_sem.at[3]),
    ]
    for copy in load_rest:
        copy.start()

    barrier = pltpu.get_barrier_semaphore()
    pl.semaphore_signal(barrier, inc=1, device_id={"dp": dp, "tensor": mate}, device_id_type=MESH)
    greeted = 1
    for i in range(1, chips):
        other = lax.rem(chip + i, chips) * 2 + core
        pl.semaphore_signal(barrier, inc=1, device_id={"dp": dp, "tensor": other}, device_id_type=MESH)
        greeted += 1

    lower, upper = dp >= 2, dp + 2 < replicas
    degree = 1 + lower.astype(jnp.int32) + upper.astype(jnp.int32)

    def greet(semaphore):
        pl.semaphore_signal(semaphore, inc=1, device_id={"dp": dp + 1 - 2 * lax.rem(dp, 2), "tensor": tensor},
                            device_id_type=MESH)

        @pl.when(lower)
        def _():
            pl.semaphore_signal(semaphore, inc=1, device_id={"dp": dp - 2, "tensor": tensor}, device_id_type=MESH)

        @pl.when(upper)
        def _():
            pl.semaphore_signal(semaphore, inc=1, device_id={"dp": dp + 2, "tensor": tensor}, device_id_type=MESH)

    rounds = replicas // 2 - 1 if reduce_dp else 0
    if reduce_dp:
        greet(barrier)
        greeted += degree

    load_ctx.wait()
    lhs[pl.ds(0, half)] = ctx[pl.ds(theirs, half)]
    lhs[pl.ds(half, half)] = ctx[pl.ds(mine, half)]

    def to_mate(j):
        span = pl.ds(j * cols, cols)
        return pltpu.make_async_remote_copy(
            src_ref=psend.at[:, span], dst_ref=precv.at[:, span], send_sem=p_send.at[j], recv_sem=p_recv.at[j],
            device_id={"dp": dp, "tensor": mate}, device_id_type=MESH)

    for j in range(count):
        span = pl.ds(j * cols, cols)
        loads_w[j].wait()
        product = jnp.dot(lhs[...], w[:, span], preferred_element_type=F32)
        psend[:, span] = product[:half].astype(BF16)
        own[:, span] = product[half:]
        if j == 0:
            pl.semaphore_wait(barrier, greeted)
            if rounds:
                greet(ladder.at[0])
        to_mate(j).start()

    def across(i, piece):
        other = lax.rem(chip + i, chips) * 2 + core
        if piece < count:
            block = ysum.at[chip, pl.ds(0, ROWS), pl.ds(piece * cols, cols)]
        else:
            block = ysum.at[chip, pl.ds((piece - count + 1) * ROWS, ROWS)]
        return pltpu.make_async_remote_copy(
            src_ref=block, dst_ref=block, send_sem=y_send.at[i - 1, piece], recv_sem=y_recv.at[i - 1, piece],
            device_id={"dp": dp, "tensor": other}, device_id_type=MESH)

    total = count + chunks - 1
    for j in range(count):
        span = pl.ds(j * cols, cols)
        to_mate(j).wait_recv()
        ysum[chip, :, span] = (own[:, span] + precv[:, span].astype(F32)).astype(BF16)
        for i in range(1, chips):
            across(i, j).start()
    for piece in range(count, total):
        for i in range(1, chips):
            across(i, piece).start()

    square = (bucket, bucket)
    diagonal = lax.broadcasted_iota(jnp.int32, square, 0) == lax.broadcasted_iota(jnp.int32, square, 1)
    order = jnp.sum(jnp.where(diagonal, slot_ref[...].astype(F32), 0.0), axis=1, keepdims=True)
    place = lax.broadcasted_iota(jnp.int32, (bucket, ctx.shape[1]), 1).astype(F32)
    chosen = jnp.where(place == order, 1.0, 0.0).astype(BF16)
    picked = lax.dot_general(chosen, ctx[...], (((1,), (1,)), ((), ())),
                             preferred_element_type=F32).astype(BF16)

    def share(r):
        span = pl.ds(mine + r * ROWS, ROWS)
        return pltpu.make_async_remote_copy(
            src_ref=resid.at[span], dst_ref=resid.at[span], send_sem=r_send.at[r], recv_sem=r_recv.at[r],
            device_id={"dp": dp, "tensor": mate}, device_id_type=MESH)

    for copy in load_rest:
        copy.wait()
    for r in range(chunks):
        for piece in (range(count) if r == 0 else (count + r - 1,)):
            for i in range(1, chips):
                across(i, piece).wait_recv()
        span = pl.ds(r * ROWS, ROWS)
        summed = ysum[0, span].astype(F32)
        for k in range(1, chips):
            summed = summed + ysum[k, span].astype(F32)
        hidden = res[span].astype(F32) + summed
        resid[pl.ds(pl.multiple_of(mine + r * ROWS, ROWS), ROWS)] = norm_backward(hidden, cot[span], gain[...])
        share(r).start()
        for turn in range(r, rounds, chunks):
            pl.semaphore_wait(ladder.at[turn], degree)
            if turn + 1 < rounds:
                greet(ladder.at[turn + 1])
    for r in range(chunks):
        share(r).wait_recv()

    def to_peer(i):
        return pltpu.make_async_remote_copy(
            src_ref=gsend.at[i - 1], dst_ref=grecv.at[i - 1], send_sem=g_send.at[i - 1], recv_sem=g_recv.at[i - 1],
            device_id={"dp": lax.rem(dp + i, replicas), "tensor": tensor}, device_id_type=MESH)

    if reduce_dp:
        block = width // replicas
        for i in sorted(range(replicas), key=lambda i: -min(i, replicas - i)):
            span = pl.ds(pl.multiple_of(lax.rem(dp + i, replicas) * block, block), block)
            gradient = jnp.dot(picked, resid[:, span], preferred_element_type=F32)
            if i == 0:
                gown[...] = gradient
            else:
                gsend[i - 1] = gradient.astype(BF16)
                to_peer(i).start()
    else:
        for j in range(count):
            span = pl.ds(j * cols, cols)
            slots_out[:, span] = jnp.dot(picked, resid[:, span], preferred_element_type=F32)

    back = None
    for j in range(count):
        span = pl.ds(j * cols, cols)
        term = lax.dot_general(resid[:, span], w[:, span], (((1,), (1,)), ((), ())), preferred_element_type=F32)
        back = term if back is None else back + term
    ctx_out[...] = back.astype(BF16)

    if reduce_dp:
        gradient = gown[...]
        for i in range(1, replicas):
            to_peer(i).wait_recv()
            gradient = gradient + grecv[i - 1].astype(F32)
        slots_out[...] = gradient * (1.0 / replicas)
    for j in range(count):
        to_mate(j).wait_send()
    for piece in range(total):
        for i in range(1, chips):
            across(i, piece).wait_send()
    for r in range(chunks):
        share(r).wait_send()
    if reduce_dp:
        for i in range(1, replicas):
            to_peer(i).wait_send()


def store_kernel(count, *refs):
    copies = [pltpu.make_async_copy(refs[i], refs[count + i], refs[2 * count].at[i]) for i in range(count)]
    for copy in copies:
        copy.start()
    for copy in copies:
        copy.wait()


def store(*arrays):
    count = len(arrays)
    return pl.pallas_call(
        functools.partial(store_kernel, count),
        out_shape=tuple(jax.ShapeDtypeStruct(a.shape, a.dtype) for a in arrays),
        in_specs=[ANY] * count,
        out_specs=(ANY,) * count,
        scratch_shapes=[pltpu.SemaphoreType.DMA((count,))],
        compiler_params=pltpu.CompilerParams(vmem_limit_bytes=1024 * 1024),
    )(*arrays)


def body(replicas, tensors, residual, context, w_out, gain, cotangent, slot_rows):
    micro, tokens, width = residual.shape
    depth = w_out.shape[0]
    bucket = slot_rows.shape[1]
    rows = micro * tokens
    half = rows // 2
    chips = tensors // 2
    count = pieces_of(width)
    pieces = count + half // ROWS - 1
    reduce_dp = replicas % 2 == 0 and width % (replicas * LANES) == 0
    block = width // replicas if reduce_dp else LANES
    peers = max(replicas - 1, 1) if reduce_dp else 1
    dma = pltpu.SemaphoreType.DMA
    spare = 4 * bucket * (block if reduce_dp else width) + 2 * rows * (depth + width)
    slots, ctx_grad, resid = pl.pallas_call(
        functools.partial(kernel, reduce_dp, replicas, tensors),
        out_shape=(
            pltpu.VMEM((bucket, block if reduce_dp else width), F32),
            pltpu.VMEM((rows, depth), BF16),
            pltpu.VMEM((rows, width), BF16),
        ),
        in_specs=[ANY] * 5 + [VMEM],
        out_specs=(VMEM, VMEM, VMEM),
        scratch_shapes=[
            pltpu.VMEM((rows, depth), BF16),
            pltpu.VMEM((depth, width), BF16),
            pltpu.VMEM((half, width), BF16),
            pltpu.VMEM((half, width), BF16),
            pltpu.VMEM((1, width), F32),
            pltpu.VMEM((rows, depth), BF16),
            pltpu.VMEM((half, width), BF16),
            pltpu.VMEM((half, width), BF16),
            pltpu.VMEM((half, width), F32),
            pltpu.VMEM((chips, half, width), BF16),
            pltpu.VMEM((peers, bucket, block), BF16),
            pltpu.VMEM((peers, bucket, block), BF16),
            pltpu.VMEM((bucket, block), F32),
            dma((4,)), dma((count,)), dma((count,)), dma((count,)),
            dma((max(chips - 1, 1), pieces)), dma((max(chips - 1, 1), pieces)),
            dma((half // ROWS,)), dma((half // ROWS,)), dma((peers,)), dma((peers,)),
            pltpu.SemaphoreType.REGULAR((max(replicas // 2 - 1, 1) if reduce_dp else 1,)),
        ],
        compiler_params=pltpu.CompilerParams(
            collective_id=0, has_side_effects=True, vmem_limit_bytes=VMEM_BYTES - spare),
    )(residual.reshape(rows, width), context.reshape(rows, depth), w_out, gain.reshape(1, width),
      cotangent.reshape(rows, width), slot_rows)
    slots, ctx_grad, resid = store(slots, ctx_grad, resid)
    if not reduce_dp:
        slots = lax.psum_scatter(slots, "dp", scatter_dimension=1, tiled=True) / replicas
    return (slots.T[None], ctx_grad.reshape(micro, tokens, depth), resid.reshape(micro, tokens, width))


def solution(mesh):
    in_specs = (
        P(None, "dp", None),
        P(None, "dp", "tensor"),
        P("tensor", None),
        P(),
        P(None, "dp", None),
        P("tensor", None),
    )
    out_specs = (P("tensor", "dp", None), P(None, "dp", "tensor"), P(None, "dp", None))
    step = functools.partial(body, mesh.shape["dp"], mesh.shape["tensor"])
    return jax.shard_map(step, mesh=mesh, in_specs=in_specs, out_specs=out_specs, check_vma=False)
```

```python
import functools

import jax
import jax.numpy as jnp
from jax import lax
from jax.experimental import pallas as pl
from jax.experimental.pallas import tpu as pltpu
from jax.sharding import PartitionSpec as P

MESH = pl.DeviceIdType.MESH
ANY = pl.BlockSpec(memory_space=pl.ANY)
VMEM = pl.BlockSpec(memory_space=pltpu.VMEM)
F32 = jnp.float32
BF16 = jnp.bfloat16
LANES = 128
ROWS = 16
VMEM_BYTES = 67043328


def pieces_of(width):
    for count in (4, 2):
        if width % (count * LANES) == 0:
            return count
    return 1


def norm_backward(hidden, cot_rows, gain):
    scale = 1.0 / hidden.shape[-1]
    center = hidden - jnp.sum(hidden, axis=-1, keepdims=True) * scale
    inverse = lax.rsqrt(jnp.sum(center * center, axis=-1, keepdims=True) * scale + 1e-05)
    upstream = cot_rows.astype(F32) * gain
    mean_up = jnp.sum(upstream, axis=-1, keepdims=True) * scale
    slope = jnp.sum(upstream * center, axis=-1, keepdims=True) * scale * inverse * inverse
    return (inverse * (upstream - mean_up - center * slope)).astype(BF16)


def kernel(reduce_dp, replicas, tensors, res_hbm, ctx_hbm, w_hbm, gain_hbm, cot_hbm, slot_hbm,
           slots_out, ctx_out, resid,
           ctx, w, res, cot, gain, slot_ref, lhs, psend, precv, own, ysum, gsend, grecv, gown,
           load_sem, w_sem, p_send, p_recv, y_send, y_recv, r_send, r_recv, g_send, g_recv, ladder):
    rows, width = resid.shape
    half = rows // 2
    chips = tensors // 2
    dp = lax.axis_index("dp")
    tensor = lax.axis_index("tensor")
    chip, core = tensor // 2, tensor % 2
    mate = chip * 2 + (1 - core)
    mine = pl.multiple_of(core * half, half)
    theirs = pl.multiple_of((1 - core) * half, half)
    count = pieces_of(width)
    cols = width // count
    chunks = half // ROWS
    bucket = slot_ref.shape[1]

    load_ctx = pltpu.make_async_copy(ctx_hbm, ctx, load_sem.at[0])
    load_ctx.start()
    loads_w = []
    for j in range(count):
        span = pl.ds(j * cols, cols)
        copy = pltpu.make_async_copy(w_hbm.at[:, span], w.at[:, span], w_sem.at[j])
        copy.start()
        loads_w.append(copy)
    load_rest = [
        pltpu.make_async_copy(res_hbm.at[pl.ds(mine, half)], res, load_sem.at[1]),
        pltpu.make_async_copy(cot_hbm.at[pl.ds(mine, half)], cot, load_sem.at[2]),
        pltpu.make_async_copy(gain_hbm, gain, load_sem.at[3]),
        pltpu.make_async_copy(slot_hbm, slot_ref, load_sem.at[4]),
    ]
    for copy in load_rest:
        copy.start()

    barrier = pltpu.get_barrier_semaphore()
    pl.semaphore_signal(barrier, inc=1, device_id={"dp": dp, "tensor": mate}, device_id_type=MESH)
    greeted = 1
    for i in range(1, chips):
        other = lax.rem(chip + i, chips) * 2 + core
        pl.semaphore_signal(barrier, inc=1, device_id={"dp": dp, "tensor": other}, device_id_type=MESH)
        greeted += 1

    lower, upper = dp >= 2, dp + 2 < replicas
    degree = 1 + lower.astype(jnp.int32) + upper.astype(jnp.int32)

    def greet(semaphore):
        pl.semaphore_signal(semaphore, inc=1, device_id={"dp": dp + 1 - 2 * lax.rem(dp, 2), "tensor": tensor},
                            device_id_type=MESH)

        @pl.when(lower)
        def _():
            pl.semaphore_signal(semaphore, inc=1, device_id={"dp": dp - 2, "tensor": tensor}, device_id_type=MESH)

        @pl.when(upper)
        def _():
            pl.semaphore_signal(semaphore, inc=1, device_id={"dp": dp + 2, "tensor": tensor}, device_id_type=MESH)

    rounds = replicas // 2 - 1 if reduce_dp else 0
    if reduce_dp:
        greet(barrier)
        greeted += degree

    load_ctx.wait()
    lhs[pl.ds(0, half)] = ctx[pl.ds(theirs, half)]
    lhs[pl.ds(half, half)] = ctx[pl.ds(mine, half)]

    def to_mate(j):
        span = pl.ds(j * cols, cols)
        return pltpu.make_async_remote_copy(
            src_ref=psend.at[:, span], dst_ref=precv.at[:, span], send_sem=p_send.at[j], recv_sem=p_recv.at[j],
            device_id={"dp": dp, "tensor": mate}, device_id_type=MESH)

    for j in range(count):
        span = pl.ds(j * cols, cols)
        loads_w[j].wait()
        product = jnp.dot(lhs[...], w[:, span], preferred_element_type=F32)
        psend[:, span] = product[:half].astype(BF16)
        own[:, span] = product[half:]
        if j == 0:
            pl.semaphore_wait(barrier, greeted)
            if rounds:
                greet(ladder.at[0])
        to_mate(j).start()

    def across(i, piece):
        other = lax.rem(chip + i, chips) * 2 + core
        if piece < count:
            block = ysum.at[chip, pl.ds(0, ROWS), pl.ds(piece * cols, cols)]
        else:
            block = ysum.at[chip, pl.ds((piece - count + 1) * ROWS, ROWS)]
        return pltpu.make_async_remote_copy(
            src_ref=block, dst_ref=block, send_sem=y_send.at[i - 1, piece], recv_sem=y_recv.at[i - 1, piece],
            device_id={"dp": dp, "tensor": other}, device_id_type=MESH)

    total = count + chunks - 1
    for j in range(count):
        span = pl.ds(j * cols, cols)
        to_mate(j).wait_recv()
        ysum[chip, :, span] = (own[:, span] + precv[:, span].astype(F32)).astype(BF16)
        for i in range(1, chips):
            across(i, j).start()
    for piece in range(count, total):
        for i in range(1, chips):
            across(i, piece).start()

    for copy in load_rest:
        copy.wait()
    square = (bucket, bucket)
    diagonal = lax.broadcasted_iota(jnp.int32, square, 0) == lax.broadcasted_iota(jnp.int32, square, 1)
    order = jnp.sum(jnp.where(diagonal, slot_ref[...].astype(F32), 0.0), axis=1, keepdims=True)
    place = lax.broadcasted_iota(jnp.int32, (bucket, ctx.shape[1]), 1).astype(F32)
    chosen = jnp.where(place == order, 1.0, 0.0).astype(BF16)
    picked = lax.dot_general(chosen, ctx[...], (((1,), (1,)), ((), ())),
                             preferred_element_type=F32).astype(BF16)

    def share(r):
        span = pl.ds(mine + r * ROWS, ROWS)
        return pltpu.make_async_remote_copy(
            src_ref=resid.at[span], dst_ref=resid.at[span], send_sem=r_send.at[r], recv_sem=r_recv.at[r],
            device_id={"dp": dp, "tensor": mate}, device_id_type=MESH)

    for r in range(chunks):
        for piece in (range(count) if r == 0 else (count + r - 1,)):
            for i in range(1, chips):
                across(i, piece).wait_recv()
        span = pl.ds(r * ROWS, ROWS)
        summed = ysum[0, span].astype(F32)
        for k in range(1, chips):
            summed = summed + ysum[k, span].astype(F32)
        hidden = res[span].astype(F32) + summed
        resid[pl.ds(pl.multiple_of(mine + r * ROWS, ROWS), ROWS)] = norm_backward(hidden, cot[span], gain[...])
        share(r).start()
        for turn in range(r, rounds, chunks):
            pl.semaphore_wait(ladder.at[turn], degree)
            if turn + 1 < rounds:
                greet(ladder.at[turn + 1])
    for r in range(chunks):
        share(r).wait_recv()

    def to_peer(i):
        return pltpu.make_async_remote_copy(
            src_ref=gsend.at[i - 1], dst_ref=grecv.at[i - 1], send_sem=g_send.at[i - 1], recv_sem=g_recv.at[i - 1],
            device_id={"dp": lax.rem(dp + i, replicas), "tensor": tensor}, device_id_type=MESH)

    if reduce_dp:
        block = width // replicas
        for i in list(range(1, replicas)) + [0]:
            span = pl.ds(pl.multiple_of(lax.rem(dp + i, replicas) * block, block), block)
            gradient = jnp.dot(picked, resid[:, span], preferred_element_type=F32)
            if i == 0:
                gown[...] = gradient
            else:
                gsend[i - 1] = gradient.astype(BF16)
                to_peer(i).start()
    else:
        for j in range(count):
            span = pl.ds(j * cols, cols)
            slots_out[:, span] = jnp.dot(picked, resid[:, span], preferred_element_type=F32)

    back = None
    for j in range(count):
        span = pl.ds(j * cols, cols)
        term = lax.dot_general(resid[:, span], w[:, span], (((1,), (1,)), ((), ())), preferred_element_type=F32)
        back = term if back is None else back + term
    ctx_out[...] = back.astype(BF16)

    if reduce_dp:
        gradient = gown[...]
        for i in range(1, replicas):
            to_peer(i).wait_recv()
            gradient = gradient + grecv[i - 1].astype(F32)
        slots_out[...] = gradient * (1.0 / replicas)
    for j in range(count):
        to_mate(j).wait_send()
    for piece in range(total):
        for i in range(1, chips):
            across(i, piece).wait_send()
    for r in range(chunks):
        share(r).wait_send()
    if reduce_dp:
        for i in range(1, replicas):
            to_peer(i).wait_send()


def store_kernel(count, *refs):
    copies = [pltpu.make_async_copy(refs[i], refs[count + i], refs[2 * count].at[i]) for i in range(count)]
    for copy in copies:
        copy.start()
    for copy in copies:
        copy.wait()


def store(*arrays):
    count = len(arrays)
    return pl.pallas_call(
        functools.partial(store_kernel, count),
        out_shape=tuple(jax.ShapeDtypeStruct(a.shape, a.dtype) for a in arrays),
        in_specs=[ANY] * count,
        out_specs=(ANY,) * count,
        scratch_shapes=[pltpu.SemaphoreType.DMA((count,))],
        compiler_params=pltpu.CompilerParams(vmem_limit_bytes=1024 * 1024),
    )(*arrays)


def body(replicas, tensors, residual, context, w_out, gain, cotangent, slot_rows):
    micro, tokens, width = residual.shape
    depth = w_out.shape[0]
    bucket = slot_rows.shape[1]
    rows = micro * tokens
    half = rows // 2
    chips = tensors // 2
    count = pieces_of(width)
    pieces = count + half // ROWS - 1
    reduce_dp = replicas % 2 == 0 and width % (replicas * LANES) == 0
    block = width // replicas if reduce_dp else LANES
    peers = max(replicas - 1, 1) if reduce_dp else 1
    dma = pltpu.SemaphoreType.DMA
    spare = 4 * bucket * (block if reduce_dp else width) + 2 * rows * (depth + width)
    slots, ctx_grad, resid = pl.pallas_call(
        functools.partial(kernel, reduce_dp, replicas, tensors),
        out_shape=(
            pltpu.VMEM((bucket, block if reduce_dp else width), F32),
            pltpu.VMEM((rows, depth), BF16),
            pltpu.VMEM((rows, width), BF16),
        ),
        in_specs=[ANY] * 6,
        out_specs=(VMEM, VMEM, VMEM),
        scratch_shapes=[
            pltpu.VMEM((rows, depth), BF16),
            pltpu.VMEM((depth, width), BF16),
            pltpu.VMEM((half, width), BF16),
            pltpu.VMEM((half, width), BF16),
            pltpu.VMEM((1, width), F32),
            pltpu.VMEM((1, bucket), jnp.int32),
            pltpu.VMEM((rows, depth), BF16),
            pltpu.VMEM((half, width), BF16),
            pltpu.VMEM((half, width), BF16),
            pltpu.VMEM((half, width), F32),
            pltpu.VMEM((chips, half, width), BF16),
            pltpu.VMEM((peers, bucket, block), BF16),
            pltpu.VMEM((peers, bucket, block), BF16),
            pltpu.VMEM((bucket, block), F32),
            dma((5,)), dma((count,)), dma((count,)), dma((count,)),
            dma((max(chips - 1, 1), pieces)), dma((max(chips - 1, 1), pieces)),
            dma((half // ROWS,)), dma((half // ROWS,)), dma((peers,)), dma((peers,)),
            pltpu.SemaphoreType.REGULAR((max(replicas // 2 - 1, 1) if reduce_dp else 1,)),
        ],
        compiler_params=pltpu.CompilerParams(
            collective_id=0, has_side_effects=True, vmem_limit_bytes=VMEM_BYTES - spare),
    )(residual.reshape(rows, width), context.reshape(rows, depth), w_out, gain.reshape(1, width),
      cotangent.reshape(rows, width), slot_rows)
    slots, ctx_grad, resid = store(slots, ctx_grad, resid)
    if not reduce_dp:
        slots = lax.psum_scatter(slots, "dp", scatter_dimension=1, tiled=True) / replicas
    return (slots.T[None], ctx_grad.reshape(micro, tokens, depth), resid.reshape(micro, tokens, width))


def solution(mesh):
    in_specs = (
        P(None, "dp", None),
        P(None, "dp", "tensor"),
        P("tensor", None),
        P(),
        P(None, "dp", None),
        P("tensor", None),
    )
    out_specs = (P("tensor", "dp", None), P(None, "dp", "tensor"), P(None, "dp", None))
    step = functools.partial(body, mesh.shape["dp"], mesh.shape["tensor"])
    return jax.shard_map(step, mesh=mesh, in_specs=in_specs, out_specs=out_specs, check_vma=False)
```

```python
import functools

import jax
import jax.numpy as jnp
from jax import lax
from jax.experimental import pallas as pl
from jax.experimental.pallas import tpu as pltpu
from jax.sharding import PartitionSpec as P

MESH = pl.DeviceIdType.MESH
ANY = pl.BlockSpec(memory_space=pl.ANY)
VMEM = pl.BlockSpec(memory_space=pltpu.VMEM)
F32 = jnp.float32
BF16 = jnp.bfloat16
LANES = 128
ROWS = 16
VMEM_BYTES = 67043328


def pieces_of(width):
    for count in (5, 4, 2):
        if width % (count * LANES) == 0:
            return count
    return 1


def norm_backward(hidden, cot_rows, gain):
    scale = 1.0 / hidden.shape[-1]
    center = hidden - jnp.sum(hidden, axis=-1, keepdims=True) * scale
    inverse = lax.rsqrt(jnp.sum(center * center, axis=-1, keepdims=True) * scale + 1e-05)
    upstream = cot_rows.astype(F32) * gain
    mean_up = jnp.sum(upstream, axis=-1, keepdims=True) * scale
    slope = jnp.sum(upstream * center, axis=-1, keepdims=True) * scale * inverse * inverse
    return (inverse * (upstream - mean_up - center * slope)).astype(BF16)


def kernel(reduce_dp, replicas, tensors, res_hbm, ctx_hbm, w_hbm, gain_hbm, cot_hbm, slot_hbm,
           slots_out, ctx_out, resid,
           ctx, w, res, cot, gain, slot_ref, lhs, psend, precv, own, ysum, gsend, grecv, gown,
           load_sem, w_sem, p_send, p_recv, y_send, y_recv, r_send, r_recv, g_send, g_recv, ladder):
    rows, width = resid.shape
    half = rows // 2
    chips = tensors // 2
    dp = lax.axis_index("dp")
    tensor = lax.axis_index("tensor")
    chip, core = tensor // 2, tensor % 2
    mate = chip * 2 + (1 - core)
    mine = pl.multiple_of(core * half, half)
    theirs = pl.multiple_of((1 - core) * half, half)
    count = pieces_of(width)
    cols = width // count
    chunks = half // ROWS
    bucket = slot_ref.shape[1]

    load_ctx = pltpu.make_async_copy(ctx_hbm, ctx, load_sem.at[0])
    load_ctx.start()
    loads_w = []
    for j in range(count):
        span = pl.ds(j * cols, cols)
        copy = pltpu.make_async_copy(w_hbm.at[:, span], w.at[:, span], w_sem.at[j])
        copy.start()
        loads_w.append(copy)
    load_rest = [
        pltpu.make_async_copy(res_hbm.at[pl.ds(mine, half)], res, load_sem.at[1]),
        pltpu.make_async_copy(cot_hbm.at[pl.ds(mine, half)], cot, load_sem.at[2]),
        pltpu.make_async_copy(gain_hbm, gain, load_sem.at[3]),
        pltpu.make_async_copy(slot_hbm, slot_ref, load_sem.at[4]),
    ]
    for copy in load_rest:
        copy.start()

    barrier = pltpu.get_barrier_semaphore()
    pl.semaphore_signal(barrier, inc=1, device_id={"dp": dp, "tensor": mate}, device_id_type=MESH)
    greeted = 1
    for i in range(1, chips):
        other = lax.rem(chip + i, chips) * 2 + core
        pl.semaphore_signal(barrier, inc=1, device_id={"dp": dp, "tensor": other}, device_id_type=MESH)
        greeted += 1

    lower, upper = dp >= 2, dp + 2 < replicas
    degree = 1 + lower.astype(jnp.int32) + upper.astype(jnp.int32)

    def greet(semaphore):
        pl.semaphore_signal(semaphore, inc=1, device_id={"dp": dp + 1 - 2 * lax.rem(dp, 2), "tensor": tensor},
                            device_id_type=MESH)

        @pl.when(lower)
        def _():
            pl.semaphore_signal(semaphore, inc=1, device_id={"dp": dp - 2, "tensor": tensor}, device_id_type=MESH)

        @pl.when(upper)
        def _():
            pl.semaphore_signal(semaphore, inc=1, device_id={"dp": dp + 2, "tensor": tensor}, device_id_type=MESH)

    rounds = replicas // 2 - 1 if reduce_dp else 0
    if reduce_dp:
        greet(barrier)
        greeted += degree

    load_ctx.wait()
    lhs[pl.ds(0, half)] = ctx[pl.ds(theirs, half)]
    lhs[pl.ds(half, half)] = ctx[pl.ds(mine, half)]

    def to_mate(j):
        span = pl.ds(j * cols, cols)
        return pltpu.make_async_remote_copy(
            src_ref=psend.at[:, span], dst_ref=precv.at[:, span], send_sem=p_send.at[j], recv_sem=p_recv.at[j],
            device_id={"dp": dp, "tensor": mate}, device_id_type=MESH)

    for j in range(count):
        span = pl.ds(j * cols, cols)
        loads_w[j].wait()
        product = jnp.dot(lhs[...], w[:, span], preferred_element_type=F32)
        psend[:, span] = product[:half].astype(BF16)
        own[:, span] = product[half:]
        if j == 0:
            pl.semaphore_wait(barrier, greeted)
        to_mate(j).start()
        if j == 0 and rounds:
            greet(ladder.at[0])

    def across(i, piece):
        other = lax.rem(chip + i, chips) * 2 + core
        if piece < count:
            block = ysum.at[chip, pl.ds(0, ROWS), pl.ds(piece * cols, cols)]
        else:
            block = ysum.at[chip, pl.ds((piece - count + 1) * ROWS, ROWS)]
        return pltpu.make_async_remote_copy(
            src_ref=block, dst_ref=block, send_sem=y_send.at[i - 1, piece], recv_sem=y_recv.at[i - 1, piece],
            device_id={"dp": dp, "tensor": other}, device_id_type=MESH)

    total = count + chunks - 1
    for j in range(count):
        span = pl.ds(j * cols, cols)
        to_mate(j).wait_recv()
        ysum[chip, :, span] = (own[:, span] + precv[:, span].astype(F32)).astype(BF16)
        for i in range(1, chips):
            across(i, j).start()
    for piece in range(count, total):
        for i in range(1, chips):
            across(i, piece).start()

    for copy in load_rest:
        copy.wait()
    square = (bucket, bucket)
    diagonal = lax.broadcasted_iota(jnp.int32, square, 0) == lax.broadcasted_iota(jnp.int32, square, 1)
    order = jnp.sum(jnp.where(diagonal, slot_ref[...].astype(F32), 0.0), axis=1, keepdims=True)
    place = lax.broadcasted_iota(jnp.int32, (bucket, ctx.shape[1]), 1).astype(F32)
    chosen = jnp.where(place == order, 1.0, 0.0).astype(BF16)
    picked = lax.dot_general(chosen, ctx[...], (((1,), (1,)), ((), ())),
                             preferred_element_type=F32).astype(BF16)

    def share(r):
        span = pl.ds(mine + r * ROWS, ROWS)
        return pltpu.make_async_remote_copy(
            src_ref=resid.at[span], dst_ref=resid.at[span], send_sem=r_send.at[r], recv_sem=r_recv.at[r],
            device_id={"dp": dp, "tensor": mate}, device_id_type=MESH)

    for r in range(chunks):
        for piece in (range(count) if r == 0 else (count + r - 1,)):
            for i in range(1, chips):
                across(i, piece).wait_recv()
        span = pl.ds(r * ROWS, ROWS)
        summed = ysum[0, span].astype(F32)
        for k in range(1, chips):
            summed = summed + ysum[k, span].astype(F32)
        hidden = res[span].astype(F32) + summed
        resid[pl.ds(pl.multiple_of(mine + r * ROWS, ROWS), ROWS)] = norm_backward(hidden, cot[span], gain[...])
        share(r).start()
        for turn in range(r * rounds // chunks, (r + 1) * rounds // chunks):
            pl.semaphore_wait(ladder.at[turn], degree)
            if turn + 1 < rounds:
                greet(ladder.at[turn + 1])
    for r in range(chunks):
        share(r).wait_recv()

    def to_peer(i):
        return pltpu.make_async_remote_copy(
            src_ref=gsend.at[i - 1], dst_ref=grecv.at[i - 1], send_sem=g_send.at[i - 1], recv_sem=g_recv.at[i - 1],
            device_id={"dp": lax.rem(dp + i, replicas), "tensor": tensor}, device_id_type=MESH)

    if reduce_dp:
        block = width // replicas
        for i in list(range(1, replicas)) + [0]:
            span = pl.ds(pl.multiple_of(lax.rem(dp + i, replicas) * block, block), block)
            gradient = jnp.dot(picked, resid[:, span], preferred_element_type=F32)
            if i == 0:
                gown[...] = gradient
            else:
                gsend[i - 1] = gradient.astype(BF16)
                to_peer(i).start()
    else:
        for j in range(count):
            span = pl.ds(j * cols, cols)
            slots_out[:, span] = jnp.dot(picked, resid[:, span], preferred_element_type=F32)

    back = None
    for j in range(count):
        span = pl.ds(j * cols, cols)
        term = lax.dot_general(resid[:, span], w[:, span], (((1,), (1,)), ((), ())), preferred_element_type=F32)
        back = term if back is None else back + term
    ctx_out[...] = back.astype(BF16)

    if reduce_dp:
        gradient = gown[...]
        for i in range(1, replicas):
            to_peer(i).wait_recv()
            gradient = gradient + grecv[i - 1].astype(F32)
        slots_out[...] = gradient * (1.0 / replicas)
    for j in range(count):
        to_mate(j).wait_send()
    for piece in range(total):
        for i in range(1, chips):
            across(i, piece).wait_send()
    for r in range(chunks):
        share(r).wait_send()
    if reduce_dp:
        for i in range(1, replicas):
            to_peer(i).wait_send()


def store_kernel(count, *refs):
    copies = [pltpu.make_async_copy(refs[i], refs[count + i], refs[2 * count].at[i]) for i in range(count)]
    for copy in copies:
        copy.start()
    for copy in copies:
        copy.wait()


def store(*arrays):
    count = len(arrays)
    return pl.pallas_call(
        functools.partial(store_kernel, count),
        out_shape=tuple(jax.ShapeDtypeStruct(a.shape, a.dtype) for a in arrays),
        in_specs=[ANY] * count,
        out_specs=(ANY,) * count,
        scratch_shapes=[pltpu.SemaphoreType.DMA((count,))],
        compiler_params=pltpu.CompilerParams(vmem_limit_bytes=1024 * 1024),
    )(*arrays)


def body(replicas, tensors, residual, context, w_out, gain, cotangent, slot_rows):
    micro, tokens, width = residual.shape
    depth = w_out.shape[0]
    bucket = slot_rows.shape[1]
    rows = micro * tokens
    half = rows // 2
    chips = tensors // 2
    count = pieces_of(width)
    pieces = count + half // ROWS - 1
    reduce_dp = replicas % 2 == 0 and width % (replicas * LANES) == 0
    block = width // replicas if reduce_dp else LANES
    peers = max(replicas - 1, 1) if reduce_dp else 1
    dma = pltpu.SemaphoreType.DMA
    spare = 4 * bucket * (block if reduce_dp else width) + 2 * rows * (depth + width)
    slots, ctx_grad, resid = pl.pallas_call(
        functools.partial(kernel, reduce_dp, replicas, tensors),
        out_shape=(
            pltpu.VMEM((bucket, block if reduce_dp else width), F32),
            pltpu.VMEM((rows, depth), BF16),
            pltpu.VMEM((rows, width), BF16),
        ),
        in_specs=[ANY] * 6,
        out_specs=(VMEM, VMEM, VMEM),
        scratch_shapes=[
            pltpu.VMEM((rows, depth), BF16),
            pltpu.VMEM((depth, width), BF16),
            pltpu.VMEM((half, width), BF16),
            pltpu.VMEM((half, width), BF16),
            pltpu.VMEM((1, width), F32),
            pltpu.VMEM((1, bucket), jnp.int32),
            pltpu.VMEM((rows, depth), BF16),
            pltpu.VMEM((half, width), BF16),
            pltpu.VMEM((half, width), BF16),
            pltpu.VMEM((half, width), F32),
            pltpu.VMEM((chips, half, width), BF16),
            pltpu.VMEM((peers, bucket, block), BF16),
            pltpu.VMEM((peers, bucket, block), BF16),
            pltpu.VMEM((bucket, block), F32),
            dma((5,)), dma((count,)), dma((count,)), dma((count,)),
            dma((max(chips - 1, 1), pieces)), dma((max(chips - 1, 1), pieces)),
            dma((half // ROWS,)), dma((half // ROWS,)), dma((peers,)), dma((peers,)),
            pltpu.SemaphoreType.REGULAR((max(replicas // 2 - 1, 1) if reduce_dp else 1,)),
        ],
        compiler_params=pltpu.CompilerParams(
            collective_id=0, has_side_effects=True, vmem_limit_bytes=VMEM_BYTES - spare),
    )(residual.reshape(rows, width), context.reshape(rows, depth), w_out, gain.reshape(1, width),
      cotangent.reshape(rows, width), slot_rows)
    slots, ctx_grad, resid = store(slots, ctx_grad, resid)
    if not reduce_dp:
        slots = lax.psum_scatter(slots, "dp", scatter_dimension=1, tiled=True) / replicas
    return (slots.T[None], ctx_grad.reshape(micro, tokens, depth), resid.reshape(micro, tokens, width))


def solution(mesh):
    in_specs = (
        P(None, "dp", None),
        P(None, "dp", "tensor"),
        P("tensor", None),
        P(),
        P(None, "dp", None),
        P("tensor", None),
    )
    out_specs = (P("tensor", "dp", None), P(None, "dp", "tensor"), P(None, "dp", None))
    step = functools.partial(body, mesh.shape["dp"], mesh.shape["tensor"])
    return jax.shard_map(step, mesh=mesh, in_specs=in_specs, out_specs=out_specs, check_vma=False)
```
